32 devices in a mesh: tp: 4 (over z), dp: 8 (over y, x, core).
Axes of the slice: x: 2, y: 2, z: 4, core: 2. Of those that a mesh axis runs over, the one named last changes fastest.
Arguments:
- x_in: bfloat16 [2048, 4096], P(('dp', 'tp'))
- w_gate: bfloat16 [4096, 14336], P('dp', 'tp')
- w_up: bfloat16 [4096, 14336], P('dp', 'tp')
- w_down: bfloat16 [14336, 4096], P('tp', 'dp')
- grad_y: bfloat16 [2048, 4096], P(('dp', 'tp'))
Outputs:
- output 1: bfloat16 [2048, 4096], P(('dp', 'tp'))
- output 2: bfloat16 [2048, 4096], P(('dp', 'tp'))
- output 3: float32 [4096, 14336], P('dp', 'tp')
- output 4: float32 [4096, 14336], P('dp', 'tp')
- output 5: float32 [14336, 4096], P('tp', 'dp')
All inputs are finite; a program needn't handle non-finite values.
Results may differ from the reference program's by a relative error of at most 0.001.
Values are sent between devices in bfloat16 or wider.
A program may use at most 1 GiB of HBM per device.

```python
import jax
import jax.numpy as jnp

D = 4096
FF = 14336
TOKENS = 2048


def setup_inputs(seed: int = 0) -> dict:
    base_key = jax.random.key(seed)
    key_list = jax.random.split(base_key, 5)
    x_in = jax.random.normal(key_list[0], (TOKENS, D), jnp.float32).astype(jnp.bfloat16)
    w_gate = (jax.random.normal(key_list[1], (D, FF), jnp.float32) * D ** -0.5).astype(jnp.bfloat16)
    w_up = (jax.random.normal(key_list[2], (D, FF), jnp.float32) * D ** -0.5).astype(jnp.bfloat16)
    w_down = (jax.random.normal(key_list[3], (FF, D), jnp.float32) * FF ** -0.5).astype(jnp.bfloat16)
    grad_y = jax.random.normal(key_list[4], (TOKENS, D), jnp.float32).astype(jnp.bfloat16)
    return {"x_in": x_in, "w_gate": w_gate, "w_up": w_up, "w_down": w_down, "grad_y": grad_y}


def reference(x_in, w_gate, w_up, w_down, grad_y):
    gate_pre = jnp.dot(x_in, w_gate, preferred_element_type=jnp.float32)
    up_pre = jnp.dot(x_in, w_up, preferred_element_type=jnp.float32)
    sig_gate = jax.nn.sigmoid(gate_pre)
    silu_gate = gate_pre * sig_gate
    hidden = (silu_gate * up_pre).astype(jnp.bfloat16)
    y_out = (x_in.astype(jnp.float32) + jnp.dot(hidden, w_down, preferred_element_type=jnp.float32)).astype(jnp.bfloat16)
    grad_h = jnp.dot(grad_y, w_down.T, preferred_element_type=jnp.float32)
    silu_deriv = sig_gate * (1.0 + gate_pre * (1.0 - sig_gate))
    grad_gate = (grad_h * up_pre * silu_deriv).astype(jnp.bfloat16)
    grad_up = (grad_h * silu_gate).astype(jnp.bfloat16)
    grad_x = (grad_y.astype(jnp.float32)
              + jnp.dot(grad_gate, w_gate.T, preferred_element_type=jnp.float32)
              + jnp.dot(grad_up, w_up.T, preferred_element_type=jnp.float32)).astype(jnp.bfloat16)
    grad_w_gate = jnp.dot(x_in.T, grad_gate, preferred_element_type=jnp.float32)
    grad_w_up = jnp.dot(x_in.T, grad_up, preferred_element_type=jnp.float32)
    grad_w_down = jnp.dot(hidden.T, grad_y, preferred_element_type=jnp.float32)
    return (y_out, grad_x, grad_w_gate, grad_w_up, grad_w_down)
```

```python
import jax
import jax.numpy as jnp
from jax import lax
from jax.sharding import PartitionSpec as P


def solution(mesh):
    dp_size = mesh.shape["dp"]
    tp_size = mesh.shape["tp"]
    flip = {o: [(i, i ^ o) for i in range(dp_size)] for o in (1, 2, 4, 6)}
    bf16, f32 = jnp.bfloat16, jnp.float32

    def swap(v, o):
        return lax.ppermute(v, "dp", flip[o])

    def local_step(x_loc, wg_loc, wu_loc, wd_loc, gy_loc):
        me = lax.axis_index("dp")
        tz = lax.axis_index("tp")
        core = me % 2
        chip = me // 2
        tok, d_model = x_loc.shape
        d_loc, ff_loc = wg_loc.shape
        fq = ff_loc // 4

        def spread_rows(rows):
            full = lax.all_gather(rows, ("tp", "dp"), axis=0, tiled=True)
            full = full.reshape(tp_size, 2, 2, 2, tok, d_model)
            own = lax.dynamic_index_in_dim(full, core, 3, keepdims=False)
            own = own.transpose(1, 0, 2, 3, 4).reshape(2, 8 * tok, d_model)
            cols = lax.dynamic_slice_in_dim(full, me * d_loc, d_loc, 5)
            cols = cols.transpose(1, 3, 0, 2, 4, 5)
            return own, cols

        def take_weight(w, f_axis, d_axis):
            def piece(o):
                return lax.dynamic_slice_in_dim(w, (chip ^ (o // 2)) * fq, fq, f_axis)

            shape = [0, 0]
            shape[f_axis] = fq
            shape[d_axis] = d_loc * dp_size
            out = jnp.zeros(shape, w.dtype)

            def put(out, v, o):
                start = [0, 0]
                start[d_axis] = (me ^ o) * d_loc
                return lax.dynamic_update_slice(out, v, tuple(start))

            mine = piece(0)
            got = {0: mine}
            for o in (2, 4, 6):
                got[o] = swap(piece(o), o)
            for o in (0, 2, 4, 6):
                out = put(out, got[o], o)
                out = put(out, swap(got[o], 1), o ^ 1)
            return out

        def gather_pair(a, b):
            ax, bx = swap(a, 2), swap(b, 2)
            ay, by = swap(a, 4), swap(b, 4)
            axy = swap(ax, 4)
            bxy = swap(by, 2)
            got = {0: (a, b), 2: (ax, bx), 4: (ay, by), 6: (axy, bxy)}
            for o in (0, 2, 4, 6):
                got[o ^ 1] = (swap(got[o][0], 1), swap(got[o][1], 1))
            return got

        def assemble(got, idx):
            t = got[0][idx].shape[0]
            out = jnp.zeros((2, t, ff_loc), bf16)
            for o, v in got.items():
                src = me ^ o
                out = lax.dynamic_update_slice(out, v[idx][None], (src % 2, 0, (src // 2) * fq))
            return out.reshape(2 * t, ff_loc)

        def sum_z(part):
            def blk(o):
                return lax.dynamic_index_in_dim(part, (tz + o) % tp_size, 2, keepdims=False)

            total = blk(0)
            for o in range(1, tp_size):
                perm = [(i, (i + o) % tp_size) for i in range(tp_size)]
                total = total + lax.ppermute(blk(o), "tp", perm)
            return total

        def finish(total, cols):
            resid = lax.dynamic_index_in_dim(cols, tz, 2, keepdims=False)
            s = total.reshape(2, 2, 2, tok, d_loc) + resid.astype(f32)
            s = s.astype(bf16).transpose(0, 2, 1, 3, 4).reshape(dp_size, tok, d_loc)
            s = lax.all_to_all(s, "dp", 0, 2, tiled=True)
            return s.reshape(tok, d_model)

        wg_all = take_weight(wg_loc, 1, 0)
        wu_all = take_weight(wu_loc, 1, 0)
        wd_all = take_weight(wd_loc, 0, 1)
        x_own, x_cols = spread_rows(x_loc)
        gy_own, gy_cols = spread_rows(gy_loc)
        n_tok = 32 * tok
        x2 = x_cols.reshape(n_tok, d_loc)
        gy2 = gy_cols.reshape(n_tok, d_loc)

        xo = x_own.reshape(16 * tok, d_model)
        gate_pre = jnp.dot(xo, wg_all, preferred_element_type=f32)
        up_pre = jnp.dot(xo, wu_all, preferred_element_type=f32)
        sig = jax.nn.sigmoid(gate_pre)
        silu = gate_pre * sig
        hidden = (silu * up_pre).astype(bf16).reshape(2, 8 * tok, fq)
        got_h = gather_pair(hidden[0], hidden[1])

        grad_h = jnp.einsum("nd,fd->nf", gy_own.reshape(16 * tok, d_model), wd_all, preferred_element_type=f32)
        deriv = sig * (1.0 + gate_pre * (1.0 - sig))
        d_gate = (grad_h * up_pre * deriv).astype(bf16).reshape(2, 8 * tok, fq)
        d_up = (grad_h * silu).astype(bf16).reshape(2, 8 * tok, fq)
        got_0 = gather_pair(d_gate[0], d_up[0])
        got_1 = gather_pair(d_gate[1], d_up[1])

        h_all = jnp.concatenate([assemble(got_h, 0), assemble(got_h, 1)], axis=0)
        y_part = jnp.dot(h_all, wd_loc, preferred_element_type=f32)
        y_sum = sum_z(y_part.reshape(2, 2, tp_size, 2 * tok, d_loc))
        y_rows = finish(y_sum, x_cols)
        grad_wd = jnp.einsum("nf,nd->fd", h_all, gy2, preferred_element_type=f32)

        gates, ups, sums = [], [], []
        for got in (got_0, got_1):
            dg, du = assemble(got, 0), assemble(got, 1)
            part = (jnp.einsum("nf,df->nd", dg, wg_loc, preferred_element_type=f32)
                    + jnp.einsum("nf,df->nd", du, wu_loc, preferred_element_type=f32))
            sums.append(sum_z(part.reshape(1, 2, tp_size, 2 * tok, d_loc)))
            gates.append(dg)
            ups.append(du)
        dg_all = jnp.concatenate(gates, axis=0)
        du_all = jnp.concatenate(ups, axis=0)
        gx_rows = finish(jnp.concatenate(sums, axis=0), gy_cols)
        grad_wg = jnp.einsum("nd,nf->df", x2, dg_all, preferred_element_type=f32)
        grad_wu = jnp.einsum("nd,nf->df", x2, du_all, preferred_element_type=f32)
        return y_rows, gx_rows, grad_wg, grad_wu, grad_wd

    row_spec = P(("dp", "tp"), None)
    up_spec = P("dp", "tp")
    down_spec = P("tp", "dp")
    return jax.shard_map(local_step, mesh=mesh,
                         in_specs=(row_spec, up_spec, up_spec, down_spec, row_spec),
                         out_specs=(row_spec, row_spec, up_spec, up_spec, down_spec),
                         check_vma=False)
```

```python
import jax
import jax.numpy as jnp
from jax import lax
from jax.sharding import PartitionSpec as P


def solution(mesh):
    dp_size = mesh.shape["dp"]
    tp_size = mesh.shape["tp"]
    flip = {o: [(i, i ^ o) for i in range(dp_size)] for o in (1, 2, 4, 6)}
    bf16, f32 = jnp.bfloat16, jnp.float32

    def swap(v, o):
        return lax.ppermute(v, "dp", flip[o])

    def local_step(x_loc, wg_loc, wu_loc, wd_loc, gy_loc):
        me = lax.axis_index("dp")
        tz = lax.axis_index("tp")
        core = me % 2
        chip = me // 2
        tok, d_model = x_loc.shape
        d_loc, ff_loc = wg_loc.shape
        fq = ff_loc // 4
        half = 2 * tp_size * tok
        n_own = 2 * half

        def split_full(full):
            full = full.reshape(tp_size, 2, 2, 2, tok, d_model)
            rows = lax.dynamic_index_in_dim(full, core, 3, keepdims=False).reshape(n_own, d_model)
            cols = []
            for i in range(2):
                c = lax.dynamic_slice(full, (0, 0, 0, (core + i) % 2, 0, me * d_loc),
                                      (tp_size, 2, 2, 1, tok, d_loc))
                cols.append(c.reshape(tp_size, 2, 2 * tok, d_loc).transpose(1, 0, 2, 3))
            return rows, cols

        def quarter(w, f_axis, o):
            return lax.dynamic_slice_in_dim(w, (chip ^ (o // 2)) * fq, fq, f_axis)

        def exchange(piece):
            got = {0: piece(0)}
            for o in (2, 4, 6):
                got[o] = swap(piece(o), o)
            return got

        def place(axis, *gots):
            width, rows = gots[0][0].shape[axis], gots[0][0].shape[0]
            shape = list(gots[0][0].shape)
            shape[axis] = 4 * width
            shape[0] *= len(gots)
            out = jnp.zeros(shape, bf16)
            for o in (0, 2, 4, 6):
                for i, got in enumerate(gots):
                    start = [i * rows, 0]
                    start[axis] += (chip ^ (o // 2)) * width
                    out = lax.dynamic_update_slice(out, got[o], tuple(start))
            return out

        def near(a, b):
            return {0: a, 2: swap(a, 2), 4: swap(a, 4)}, {0: b, 4: swap(b, 4), 2: swap(b, 2)}

        def far(got_a, got_b):
            return {**got_a, 6: swap(got_a[2], 4)}, {**got_b, 6: swap(got_b[4], 2)}

        def send_z(parts):
            def blk(o):
                return jnp.stack([lax.dynamic_index_in_dim(p, (tz + o) % tp_size, 1, keepdims=False) for p in parts])

            got = [blk(0)]
            for o in (2, 1, 3):
                perm = [(i, (i + o) % tp_size) for i in range(tp_size)]
                got.append(lax.ppermute(blk(o), "tp", perm))
            return got

        def finish(total, cols):
            resid = jnp.stack([lax.dynamic_index_in_dim(c, tz, 1, keepdims=False) for c in cols])
            s = (total + resid.astype(f32)).astype(bf16)
            s = jnp.where(core == 0, s, jnp.flip(s, axis=0))
            s = s.reshape(2, 4, tok, d_loc).transpose(1, 0, 2, 3).reshape(dp_size, tok, d_loc)
            s = lax.all_to_all(s, "dp", 0, 2, tiled=True)
            return s.reshape(tok, d_model)

        def dot2(rows, ws, eq):
            return (jnp.einsum(eq, rows[0], ws[0], preferred_element_type=f32)
                    + jnp.einsum(eq, rows[1], ws[1], preferred_element_type=f32))

        x_full = lax.all_gather(x_loc, ("tp", "dp"), axis=0, tiled=True)
        gy_full = lax.all_gather(gy_loc, ("tp", "dp"), axis=0, tiled=True)
        got_gu = exchange(lambda o: jnp.concatenate([quarter(wg_loc, 1, o), quarter(wu_loc, 1, o)], axis=1))
        wd_late, got_gu[2], got_gu[4] = lax.optimization_barrier((wd_loc, got_gu[2], got_gu[4]))
        got_d = exchange(lambda o: quarter(wd_late, 0, o))

        wgu = place(0, got_gu)
        wgu = (wgu.reshape(4, d_loc, 2 * fq), swap(wgu, 1).reshape(4, d_loc, 2 * fq))
        wgu = jnp.where(core == 0, jnp.stack(wgu, axis=1), jnp.stack(wgu[::-1], axis=1)).reshape(d_model, 2 * fq)
        x_full, got_d[2], got_d[4], got_d[6] = lax.optimization_barrier((x_full, got_d[2], got_d[4], got_d[6]))
        x_rows, x_cols = split_full(x_full)
        wd_all = place(1, got_d)
        wd_pair = (wd_all, swap(wd_all, 1))
        wd_all = jnp.zeros((fq, d_model), bf16)
        for i in range(2):
            for c in range(4):
                wd_all = lax.dynamic_update_slice(wd_all, wd_pair[i][:, c * d_loc:(c + 1) * d_loc],
                                                  (0, (2 * c + (core + i) % 2) * d_loc))
        pre = jnp.dot(x_rows, wgu, preferred_element_type=f32)
        gate_pre, up_pre = pre[:, :fq], pre[:, fq:]
        sig = jax.nn.sigmoid(gate_pre)
        silu = gate_pre * sig
        hidden = (silu * up_pre).astype(bf16).reshape(tp_size, 2, 2 * tok, fq)
        got_h = far(*near(hidden[:, 0].reshape(half, fq), hidden[:, 1].reshape(half, fq)))
        h_own = place(1, *got_h)

        h_all = (h_own, swap(h_own, 1))
        y_part = [jnp.dot(h, wd_loc, preferred_element_type=f32) for h in h_all]
        gy_full, _ = lax.optimization_barrier((gy_full, y_part))
        y_got = send_z([p.reshape(2, tp_size, 2 * tok, d_loc) for p in y_part])
        gy_rows, gy_cols = split_full(gy_full)
        grad_h = jnp.einsum("nd,fd->nf", gy_rows, wd_all, preferred_element_type=f32)
        deriv = sig * (1.0 + gate_pre * (1.0 - sig))
        d_gate = (grad_h * up_pre * deriv).astype(bf16).reshape(tp_size, 2, 2 * tok, fq)
        d_up = (grad_h * silu).astype(bf16).reshape(tp_size, 2, 2 * tok, fq)
        got_0 = near(d_gate[:, 0].reshape(half, fq), d_up[:, 0].reshape(half, fq))
        got_1 = near(d_gate[:, 1].reshape(half, fq), d_up[:, 1].reshape(half, fq))
        got_0, got_1 = far(*got_0), far(*got_1)
        grad_wd = dot2(h_all, [c.reshape(n_own, d_loc) for c in gy_cols], "nf,nd->fd")

        grad_wg = grad_wu = None
        x_got = []
        for y in range(2):
            got = (got_0, got_1)[y]
            dg, du = place(1, got[0]), place(1, got[1])
            dg, du = (dg, swap(dg, 1)), (du, swap(du, 1))
            part = [jnp.einsum("nf,df->nd", dg[i], wg_loc, preferred_element_type=f32)
                    + jnp.einsum("nf,df->nd", du[i], wu_loc, preferred_element_type=f32) for i in range(2)]
            x_got.append(send_z([p.reshape(1, tp_size, 2 * tok, d_loc) for p in part]))
            xc = [c[y].reshape(half, d_loc) for c in x_cols]
            part_g = dot2(xc, dg, "nd,nf->df")
            part_u = dot2(xc, du, "nd,nf->df")
            grad_wg = part_g if grad_wg is None else grad_wg + part_g
            grad_wu = part_u if grad_wu is None else grad_wu + part_u
        y_rows = finish(sum(y_got[1:], y_got[0]), x_cols)
        x_got = [sum(g[1:], g[0]) for g in x_got]
        gx_rows = finish(jnp.concatenate(x_got, axis=1), gy_cols)
        return y_rows, gx_rows, grad_wg, grad_wu, grad_wd


    row_spec = P(("dp", "tp"), None)
    up_spec = P("dp", "tp")
    down_spec = P("tp", "dp")
    return jax.shard_map(local_step, mesh=mesh,
                         in_specs=(row_spec, up_spec, up_spec, down_spec, row_spec),
                         out_specs=(row_spec, row_spec, up_spec, up_spec, down_spec),
                         check_vma=False)
```

```python
import jax
import jax.numpy as jnp
from jax import lax
from jax.sharding import PartitionSpec as P


def solution(mesh):
    dp_size = mesh.shape["dp"]
    tp_size = mesh.shape["tp"]
    flip = {o: [(i, i ^ o) for i in range(dp_size)] for o in (1, 2, 4, 6)}
    bf16, f32 = jnp.bfloat16, jnp.float32

    def swap(v, o):
        return lax.ppermute(v, "dp", flip[o])

    def local_step(x_loc, wg_loc, wu_loc, wd_loc, gy_loc):
        me = lax.axis_index("dp")
        tz = lax.axis_index("tp")
        core = me % 2
        chip = me // 2
        tok, d_model = x_loc.shape
        d_loc, ff_loc = wg_loc.shape
        fq = ff_loc // 4
        half = 2 * tp_size * tok
        n_own = 2 * half

        def split_full(full):
            full = full.reshape(tp_size, 2, 2, 2, tok, d_model)
            rows = lax.dynamic_index_in_dim(full, core, 3, keepdims=False).reshape(n_own, d_model)
            cols = []
            for i in range(2):
                c = lax.dynamic_slice(full, (0, 0, 0, (core + i) % 2, 0, me * d_loc),
                                      (tp_size, 2, 2, 1, tok, d_loc))
                cols.append(c.reshape(tp_size, 2, 2 * tok, d_loc).transpose(1, 0, 2, 3))
            return rows, cols

        def quarter(w, f_axis, o):
            return lax.dynamic_slice_in_dim(w, (chip ^ (o // 2)) * fq, fq, f_axis)

        def exchange(piece):
            got = {0: piece(0)}
            for o in (2, 4, 6):
                got[o] = swap(piece(o), o)
            return got

        def place(axis, *gots):
            width, rows = gots[0][0].shape[axis], gots[0][0].shape[0]
            shape = list(gots[0][0].shape)
            shape[axis] = 4 * width
            shape[0] *= len(gots)
            out = jnp.zeros(shape, bf16)
            for o in (0, 2, 4, 6):
                for i, got in enumerate(gots):
                    start = [i * rows, 0]
                    start[axis] += (chip ^ (o // 2)) * width
                    out = lax.dynamic_update_slice(out, got[o], tuple(start))
            return out

        def near(a, b):
            return {0: a, 2: swap(a, 2), 4: swap(a, 4)}, {0: b, 4: swap(b, 4), 2: swap(b, 2)}

        def far(got_a, got_b):
            return {**got_a, 6: swap(got_a[2], 4)}, {**got_b, 6: swap(got_b[4], 2)}

        def send_z(parts):
            def blk(o):
                return jnp.stack([lax.dynamic_index_in_dim(p, (tz + o) % tp_size, 1, keepdims=False) for p in parts])

            got = [blk(0)]
            for o in (2, 1, 3):
                perm = [(i, (i + o) % tp_size) for i in range(tp_size)]
                got.append(lax.ppermute(blk(o), "tp", perm))
            return got

        def finish(total, cols):
            resid = jnp.stack([lax.dynamic_index_in_dim(c, tz, 1, keepdims=False) for c in cols])
            s = (total + resid.astype(f32)).astype(bf16)
            s = jnp.where(core == 0, s, jnp.flip(s, axis=0))
            s = s.reshape(2, 4, tok, d_loc).transpose(1, 0, 2, 3).reshape(dp_size, tok, d_loc)
            s = lax.all_to_all(s, "dp", 0, 2, tiled=True)
            return s.reshape(tok, d_model)

        def dot2(rows, ws, eq):
            return (jnp.einsum(eq, rows[0], ws[0], preferred_element_type=f32)
                    + jnp.einsum(eq, rows[1], ws[1], preferred_element_type=f32))

        x_full = lax.all_gather(x_loc, ("tp", "dp"), axis=0, tiled=True)
        hd = d_model // 2
        gy_full = lax.all_gather(gy_loc[:, :hd], ("tp", "dp"), axis=0, tiled=True)
        gyb = exchange(lambda o: gy_loc[:, hd:])
        gyb = place(0, gyb)
        gyb_got = []
        for o in (2, 1, 3):
            gyb_got.append((o, lax.ppermute(gyb, "tp", [(i, (i + o) % tp_size) for i in range(tp_size)])))
        gyb_rows = jnp.zeros((n_own, hd), bf16)
        for o, v in [(0, gyb)] + gyb_got:
            start = ((tz + tp_size - o) % tp_size) * (4 * tok)
            gyb_rows = lax.dynamic_update_slice(gyb_rows, v, (start, 0))
        got_gu = exchange(lambda o: jnp.concatenate([quarter(wg_loc, 1, o), quarter(wu_loc, 1, o)], axis=1))
        got_d = exchange(lambda o: quarter(wd_loc, 0, o))

        wgu = place(0, got_gu)
        wgu = (wgu.reshape(4, d_loc, 2 * fq), swap(wgu, 1).reshape(4, d_loc, 2 * fq))
        wgu = jnp.where(core == 0, jnp.stack(wgu, axis=1), jnp.stack(wgu[::-1], axis=1)).reshape(d_model, 2 * fq)
        x_rows, x_cols = split_full(x_full)
        wd_all = place(1, got_d)
        wd_pair = (wd_all, swap(wd_all, 1))
        wd_all = [jnp.zeros((fq, hd), bf16) for _ in range(2)]
        for i in range(2):
            for c in range(4):
                wd_all[c // 2] = lax.dynamic_update_slice(wd_all[c // 2], wd_pair[i][:, c * d_loc:(c + 1) * d_loc],
                                                          (0, (2 * (c % 2) + (core + i) % 2) * d_loc))
        pre = jnp.dot(x_rows, wgu, preferred_element_type=f32)
        gate_pre, up_pre = pre[:, :fq], pre[:, fq:]
        sig = jax.nn.sigmoid(gate_pre)
        silu = gate_pre * sig
        hidden = (silu * up_pre).astype(bf16).reshape(tp_size, 2, 2 * tok, fq)
        got_h = near(hidden[:, 0].reshape(half, fq), hidden[:, 1].reshape(half, fq))
        got_h = far(*got_h)
        h_own = place(1, *got_h)

        gy_full, gyb_rows, _ = lax.optimization_barrier((gy_full, gyb_rows, hidden))
        h_all = (h_own, swap(h_own, 1))
        y_part = [jnp.dot(h, wd_loc, preferred_element_type=f32) for h in h_all]
        y_got = send_z([p.reshape(2, tp_size, 2 * tok, d_loc) for p in y_part])
        gya_rows = gy_full.reshape(tp_size, 2, 2, 2, tok, hd)
        gya_rows = lax.dynamic_index_in_dim(gya_rows, core, 3, keepdims=False).reshape(n_own, hd)

        def gy_col(dev):
            start = (dev % 4) * d_loc
            return jnp.where(dev < 4, lax.dynamic_slice_in_dim(gya_rows, start, d_loc, 1),
                             lax.dynamic_slice_in_dim(gyb_rows, start, d_loc, 1))

        gy_cols = [gy_col(me), swap(gy_col(me ^ 1), 1)]
        gy_cols = [c.reshape(tp_size, 2, 2 * tok, d_loc).transpose(1, 0, 2, 3) for c in gy_cols]
        grad_h = dot2((gya_rows, gyb_rows), wd_all, "nd,fd->nf")
        deriv = sig * (1.0 + gate_pre * (1.0 - sig))
        d_gate = (grad_h * up_pre * deriv).astype(bf16).reshape(tp_size, 2, 2 * tok, fq)
        d_up = (grad_h * silu).astype(bf16).reshape(tp_size, 2, 2 * tok, fq)
        got_0 = near(d_gate[:, 0].reshape(half, fq), d_up[:, 0].reshape(half, fq))
        got_1 = near(d_gate[:, 1].reshape(half, fq), d_up[:, 1].reshape(half, fq))
        got_0 = far(*got_0)
        got_1 = far(*got_1)
        grad_wd = dot2(h_all, [c.reshape(n_own, d_loc) for c in gy_cols], "nf,nd->fd")

        grad_wg = grad_wu = None
        x_got = []
        for y in range(2):
            got = (got_0, got_1)[y]
            dg, du = place(1, got[0]), place(1, got[1])
            dg, du = (dg, swap(dg, 1)), (du, swap(du, 1))
            part = [jnp.einsum("nf,df->nd", dg[i], wg_loc, preferred_element_type=f32)
                    + jnp.einsum("nf,df->nd", du[i], wu_loc, preferred_element_type=f32) for i in range(2)]
            x_got.append(send_z([p.reshape(1, tp_size, 2 * tok, d_loc) for p in part]))
            xc = [c[y].reshape(half, d_loc) for c in x_cols]
            for i in range(2):
                part_g = jnp.einsum("nd,nf->df", xc[i], dg[i], preferred_element_type=f32)
                part_u = jnp.einsum("nd,nf->df", xc[i], du[i], preferred_element_type=f32)
                grad_wg = part_g if grad_wg is None else grad_wg + part_g
                grad_wu = part_u if grad_wu is None else grad_wu + part_u
        y_rows = finish(sum(y_got[1:], y_got[0]), x_cols)
        x_got = [sum(g[1:], g[0]) for g in x_got]
        gx_rows = finish(jnp.concatenate(x_got, axis=1), gy_cols)
        return y_rows, gx_rows, grad_wg, grad_wu, grad_wd


    row_spec = P(("dp", "tp"), None)
    up_spec = P("dp", "tp")
    down_spec = P("tp", "dp")
    return jax.shard_map(local_step, mesh=mesh,
                         in_specs=(row_spec, up_spec, up_spec, down_spec, row_spec),
                         out_specs=(row_spec, row_spec, up_spec, up_spec, down_spec),
                         check_vma=False)
```
